32 devices in a mesh: gx: 8 (over y, x, core), gy: 4 (over z).
Axes of the slice: x: 2, y: 2, z: 4, core: 2. Of those that a mesh axis runs over, the one named last changes fastest.
Arguments:
- cells: int32 [3, 1048576], P(None, ('gx', 'gy')), may hold values from 0 to 255, as said below
- fractions: float32 [3, 1048576], P(None, ('gx', 'gy')), may hold values from 0 to 1
- charges: float32 [1048576], P(('gx', 'gy')), may hold values from -24 to 24
- influence: float32 [256, 256, 256], P('gx', 'gy'), may hold values from 0.05 to 24, as said below
- shells: int32 [256, 256, 256], P('gx', 'gy'), may hold values from 0 to 255
Outputs:
- potential_hat: float32 [2, 256, 256, 256], P(None, 'gx', 'gy')
- energy: float32 [], replicated
- virial: float32 [3, 3], replicated
- spectrum: float32 [256], replicated
The draws below stay inside these ranges and needn't reach their ends.
Inputs may be any that keep to these rules, and one draw needn't show every extreme that they name: `cells`: atom a belongs to device a // 32768, devices numbered with gy fastest; its y cell lies in that device's block of 32 y planes (block index its gx index) and its z cell in its block of 64 z planes (block index its gy index). `influence`: Positive.
All inputs are finite; a program needn't handle non-finite values.
Results may differ from the reference program's by a relative error of at most 0.0029.
Values sent between devices are 32-bit elements; how exact they have to be, the bound alone decides.
No kernel may reach another device: no remote copies, remote signals or barrier semaphores. Data moves between devices by JAX's collectives and lax.ppermute only.
A program may use at most 64 MiB of HBM per device.

```python
import jax
import jax.numpy as jnp
from jax import lax

MESH = 256
SHELLS = 256
SCREEN = 4096
ATOM_DEV = 32768
ATOMS = 1048576
CYD = 32
CZD = 64


def draw_cells(key, part):
    keys = jax.random.split(jax.random.fold_in(key, 11), 3)
    row_index = jnp.arange(ATOMS, dtype=jnp.int32)
    device = row_index // ATOM_DEV
    columns = MESH // CZD
    cell_x = jax.random.randint(keys[0], (ATOMS,), 0, MESH, dtype=jnp.int32)
    cell_y = device // columns * CYD + jax.random.randint(keys[1], (ATOMS,), 0, CYD, dtype=jnp.int32)
    cell_z = device % columns * CZD + jax.random.randint(keys[2], (ATOMS,), 0, CZD, dtype=jnp.int32)
    return jnp.stack([cell_x, cell_y, cell_z]).astype(jnp.int32)


def wave_squared():
    index = jnp.arange(MESH, dtype=jnp.int32)
    wave = jnp.where(index < MESH // 2, index, index - MESH).astype(jnp.float32)
    return wave[:, None, None] ** 2 + wave[None, :, None] ** 2 + wave[None, None, :] ** 2


def draw_influence(key, part):
    squared = wave_squared()
    shape = (MESH, MESH, MESH)
    rough = jnp.exp(jax.random.uniform(jax.random.fold_in(key, 22), shape, jnp.float32, -0.6931, 0.6931))
    return (rough * 8.0 / (1.0 + squared / 2048.0)).astype(jnp.float32)


def draw_shells(key, part):
    metric_tensor = jax.random.randint(jax.random.fold_in(key, 31), (3,), 1, 4, dtype=jnp.int32)
    index = jnp.arange(MESH, dtype=jnp.int32)
    wave = jnp.where(index < MESH // 2, index, index - MESH)
    radius = metric_tensor[0] * wave[:, None, None] ** 2 + metric_tensor[1] * wave[None, :, None] ** 2 + metric_tensor[2] * wave[None, None, :] ** 2
    top_value = (metric_tensor[0] + metric_tensor[1] + metric_tensor[2]) * (MESH // 2) ** 2
    return jnp.minimum(radius * SHELLS // (top_value + 1), SHELLS - 1).astype(jnp.int32)


def block_levels(rng, dims, pieces, smallest, largest):
    def one(dim, parts):
        steps = jax.random.uniform(jax.random.fold_in(jax.random.fold_in(rng, 6), dim), (parts,), jnp.float32, smallest / len(pieces), largest / len(pieces))
        return jnp.repeat(jnp.exp(steps), dims[dim] // parts).reshape((-1,) + (1,) * (len(dims) - dim - 1))

    level = one(*pieces[0])
    for cut in pieces[1:]:
        level = level * one(*cut)
    return level


def centred(rng, shape, width, most, pieces=(), kind=jnp.bfloat16):
    factor_of = block_levels(rng, shape, pieces, -0.22, 0.18) if pieces else 1.0
    values = jax.random.normal(rng, shape, jnp.float32) * width * factor_of
    return jnp.minimum(jnp.maximum(values, -most), most).astype(kind)


def setup_inputs(seed: int = 0) -> dict:
    splits = jax.random.split(jax.random.key(seed), 6)
    return {
        "cells": draw_cells(jax.random.fold_in(splits[5], 71), 0),
        "fractions": jnp.clip(1.0 * jax.random.uniform(splits[1], (3, ATOMS), jnp.float32) ** block_levels(splits[1], (3, ATOMS), ((1, 32),), -0.2, 0.2), 0.0, 1.0),
        "charges": centred(splits[2], (ATOMS,), 4.0, 24.0, ((0, 32),), jnp.float32),
        "influence": draw_influence(jax.random.fold_in(splits[5], 71), 0),
        "shells": draw_shells(jax.random.fold_in(splits[5], 71), 0),
    }


def spline(frac):
    cube = frac * frac * frac
    square = frac * frac
    rest = 1.0 - frac
    return (rest * rest * rest / 6.0, (3.0 * cube - 6.0 * square + 4.0) / 6.0, (-3.0 * cube + 3.0 * square + 3.0 * frac + 1.0) / 6.0, cube / 6.0)


def wave_numbers(index):
    return jnp.where(index < MESH // 2, index, index - MESH).astype(jnp.float32)


def reference(cells, fractions, charges, influence, shells):
    weight_x = spline(fractions[0])
    weight_y = spline(fractions[1])
    weight_z = spline(fractions[2])
    charge_mesh = jnp.zeros((MESH, MESH, MESH), jnp.float32)
    for first in range(4):
        factor_x = lax.optimization_barrier((charges * weight_x[first]).astype(jnp.bfloat16)).astype(jnp.float32)
        index_x = ((cells[0] + first) % MESH).astype(jnp.int32)
        for second in range(4):
            index_y = ((cells[1] + second) % MESH).astype(jnp.int32)
            for third in range(4):
                index_z = ((cells[2] + third) % MESH).astype(jnp.int32)
                factor_yz = lax.optimization_barrier((weight_y[second] * weight_z[third]).astype(jnp.bfloat16)).astype(jnp.float32)
                charge_mesh = charge_mesh.at[index_x, index_y, index_z].add(factor_x * factor_yz)
    transform = jnp.fft.fftn(charge_mesh) / (MESH ** 1.5)
    real_part = jnp.real(transform).astype(jnp.float32)
    imag_part = jnp.imag(transform).astype(jnp.float32)
    index = jnp.arange(MESH, dtype=jnp.int32)
    wave = wave_numbers(index)
    wave_x = wave[:, None, None]
    wave_y = wave[None, :, None]
    wave_z = wave[None, None, :]
    squared = wave_x * wave_x + wave_y * wave_y + wave_z * wave_z
    keep = jnp.where(squared > 0.0, 1.0, 0.0).astype(jnp.float32)
    weight = keep * influence
    potential_hat = jnp.stack([weight * real_part, weight * imag_part])
    power = real_part * real_part + imag_part * imag_part
    influence_weighted = weight * power
    scale = 0.5 / (MESH ** 3)
    whole_sum = jnp.sum(influence_weighted)
    energy = scale * whole_sum
    coef = influence_weighted * 2.0 * (1.0 + squared / SCREEN) / (squared + 1.0 - keep)
    waves = (wave_x, wave_y, wave_z)
    rows_out = []
    for left in range(3):
        entries = []
        for right in range(3):
            cross = jnp.sum(coef * waves[left] * waves[right])
            diagonal = whole_sum if left == right else jnp.float32(0.0)
            entries.append(scale * (diagonal - cross))
        rows_out.append(jnp.stack(entries))
    virial = jnp.stack(rows_out)
    spectrum = jax.ops.segment_sum(power.reshape(-1), shells.reshape(-1).astype(jnp.int32), num_segments=SHELLS) * (SHELLS / (MESH ** 3))
    return potential_hat, energy, virial, spectrum
```

```python
import functools

import jax
import jax.numpy as jnp
import numpy as np
from jax import lax
from jax.experimental import pallas as pl
from jax.experimental.pallas import tpu as pltpu
from jax.sharding import PartitionSpec as P

MESH = 256
SHELLS = 256
SCREEN = 4096
HALO = 3
WAVES = 8
PLANES = 16
SIDE = 16


def whole_block(shape):
    return pl.BlockSpec(shape, lambda *_: (0,) * len(shape))


def two_parts(values):
    top = values.astype(jnp.bfloat16)
    return top, (values - top.astype(jnp.float32)).astype(jnp.bfloat16)


def table_parts(table):
    top = np.asarray(table, np.float32).astype(jnp.bfloat16)
    rest = (table - top.astype(np.float64)).astype(np.float32).astype(jnp.bfloat16)
    return top, rest


def waves():
    index = np.arange(MESH)
    angle = (index[:, None] * index[None, :] % MESH) * (2.0 * np.pi / MESH)
    return np.cos(angle) / np.sqrt(MESH), np.sin(angle) / np.sqrt(MESH)


def x_table(nx):
    cosine, sine = waves()
    both = np.stack([cosine, -sine]).reshape(2, nx, MESH // nx // WAVES, WAVES, MESH)
    rows = both.transpose(1, 2, 0, 3, 4).reshape(2 * MESH, MESH)
    top, rest = table_parts(rows)
    joined = np.concatenate([top, rest, top], axis=1)
    return np.concatenate([joined, joined], axis=0)


def backward_blocks(table, parts):
    blocks = table.reshape((parts, MESH // parts) + table.shape[1:])
    order = [(-q) % parts for q in range(2 * parts)]
    return blocks[order].reshape((2 * MESH,) + table.shape[1:])


def y_table(nx, ny):
    cosine, sine = waves()
    width = MESH // ny
    full = np.stack([np.stack([cosine, -sine], 1), np.stack([sine, cosine], 1)])
    full = full.reshape(2, MESH, 2, ny, width).transpose(3, 0, 1, 2, 4)
    full = full.reshape(ny, 2, MESH, 2 * width)
    turned = np.stack(
        [np.stack([backward_blocks(full[d, c], nx) for c in range(2)]) for d in range(ny)]
    )
    return table_parts(turned)


def z_table(ny):
    cosine, sine = waves()
    return table_parts(backward_blocks(np.concatenate([cosine, sine], axis=1), ny))


def spline(frac):
    cube = frac * frac * frac
    square = frac * frac
    rest = 1.0 - frac
    return (
        rest * rest * rest / 6.0,
        (3.0 * cube - 6.0 * square + 4.0) / 6.0,
        (-3.0 * cube + 3.0 * square + 3.0 * frac + 1.0) / 6.0,
        cube / 6.0,
    )


def placed(offset, weights):
    result = jnp.where(offset == 3, weights[3], 0.0)
    for turn in (2, 1, 0):
        result = jnp.where(offset == turn, weights[turn], result)
    return result


def axis_table(cell, weights, axis, rows, first):
    count = cell.shape[1]
    index = lax.broadcasted_iota(jnp.int32, (rows, count), 0)
    offset = index - (cell[axis : axis + 1, :] - first)
    return placed(offset, [w[axis : axis + 1, :] for w in weights])


NT = (((1,), (1,)), ((), ()))


def dot_nt(a, b):
    return lax.dot_general(a, b, NT, preferred_element_type=jnp.float32)


def edge_kernel(
    plane_y, plane_z, me, cells, frac, charge, xt, edge_y, edge_z, corner, yt, zt, rows
):
    count = cells.shape[1]
    cell = cells[...]
    weights = spline(frac[...])
    charged = charge[...]
    index = lax.broadcasted_iota(jnp.int32, (MESH, count), 0)
    offset = (index - cell[0:1, :]) & (MESH - 1)
    table = placed(offset, [charged * w[0:1, :] for w in weights]).astype(jnp.bfloat16)
    xt[...] = table
    yt[...] = axis_table(cell, weights, 1, yt.shape[0], me[0] * plane_y)
    zt[...] = axis_table(cell, weights, 2, zt.shape[0], me[1] * plane_z)
    at = 0
    for d in range(HALO):
        part = yt[plane_y + d : plane_y + d + 1, :] * zt[:plane_z, :]
        rows[at : at + plane_z, :] = part.astype(jnp.bfloat16)
        at += plane_z
    for d in range(HALO):
        part = zt[plane_z + d : plane_z + d + 1, :] * yt[:plane_y, :]
        rows[at : at + plane_y, :] = part.astype(jnp.bfloat16)
        at += plane_y
    for d in range(HALO):
        part = zt[plane_z + d : plane_z + d + 1, :] * yt[plane_y : plane_y + 16, :]
        rows[at : at + 16, :] = part.astype(jnp.bfloat16)
        at += 16
    total = dot_nt(rows[...], table)

    @pl.when(pl.program_id(0) == 0)
    def _():
        edge_y[...] = jnp.zeros_like(edge_y)
        edge_z[...] = jnp.zeros_like(edge_z)
        corner[...] = jnp.zeros_like(corner)

    at = HALO * plane_z
    edge_y[...] += total[:at]
    edge_z[...] += total[at : at + HALO * plane_y]
    corner[...] += total[at + HALO * plane_y :]


def edges(me, cells, frac, charges, plane_y, plane_z):
    atoms = charges.shape[1]
    block = min(1024, atoms)
    rows = HALO * (plane_z + plane_y + 16)
    return pl.pallas_call(
        functools.partial(edge_kernel, plane_y, plane_z),
        grid=(atoms // block,),
        in_specs=[
            pl.BlockSpec(memory_space=pltpu.SMEM),
            pl.BlockSpec((3, block), lambda i: (0, i)),
            pl.BlockSpec((3, block), lambda i: (0, i)),
            pl.BlockSpec((1, block), lambda i: (0, i)),
        ],
        out_specs=[
            pl.BlockSpec((MESH, block), lambda i: (0, i)),
            whole_block((HALO * plane_z, MESH)),
            whole_block((HALO * plane_y, MESH)),
            whole_block((HALO * 16, MESH)),
        ],
        out_shape=[
            jax.ShapeDtypeStruct((MESH, atoms), jnp.bfloat16),
            jax.ShapeDtypeStruct((HALO * plane_z, MESH), jnp.float32),
            jax.ShapeDtypeStruct((HALO * plane_y, MESH), jnp.float32),
            jax.ShapeDtypeStruct((HALO * 16, MESH), jnp.float32),
        ],
        scratch_shapes=[
            pltpu.VMEM((plane_y + 16, block), jnp.float32),
            pltpu.VMEM((plane_z + 8, block), jnp.float32),
            pltpu.VMEM((rows, block), jnp.bfloat16),
        ],
        cost_estimate=pl.CostEstimate(
            flops=8 * rows * atoms * MESH, bytes_accessed=4 * MESH * atoms, transcendentals=0
        ),
        name="edges",
    )(me, cells, frac, charges)


def spread_kernel(plane_y, plane_z, me, cells, frac, xt, out, zt, pairs):
    cell = cells[...]
    weights = spline(frac[...])
    table_y = axis_table(cell, weights, 1, plane_y, me[0] * plane_y)
    zt[...] = axis_table(cell, weights, 2, plane_z, me[1] * plane_z)
    for z in range(plane_z):
        part = zt[z : z + 1, :] * table_y
        pairs[z * plane_y : (z + 1) * plane_y, :] = part.astype(jnp.bfloat16)

    @pl.when(pl.program_id(0) == 0)
    def _():
        out[...] = jnp.zeros_like(out)

    out[...] += dot_nt(pairs[...], xt[...])


def spread(me, cells, frac, xt, plane_y, plane_z):
    atoms = cells.shape[1]
    block = min(1024, atoms)
    rows = plane_y * plane_z
    return pl.pallas_call(
        functools.partial(spread_kernel, plane_y, plane_z),
        grid=(atoms // block,),
        in_specs=[
            pl.BlockSpec(memory_space=pltpu.SMEM),
            pl.BlockSpec((3, block), lambda i: (0, i)),
            pl.BlockSpec((3, block), lambda i: (0, i)),
            pl.BlockSpec((MESH, block), lambda i: (0, i)),
        ],
        out_specs=whole_block((rows, MESH)),
        out_shape=jax.ShapeDtypeStruct((rows, MESH), jnp.float32),
        scratch_shapes=[
            pltpu.VMEM((plane_z, block), jnp.float32),
            pltpu.VMEM((rows, block), jnp.bfloat16),
        ],
        cost_estimate=pl.CostEstimate(
            flops=2 * rows * atoms * MESH, bytes_accessed=4 * MESH * atoms, transcendentals=0
        ),
        name="spread",
    )(me, cells, frac, xt)


def x_kernel(nx, chunks, plane_y, me, mesh, edge_y, edge_z, corner, table, *rest):
    outs, work = rest[:-1], rest[-1]
    work[...] = mesh[...]
    for d in range(HALO):
        work[:, d, :] += edge_y[d]

    @pl.when(pl.program_id(0) == 0)
    def _():
        for d in range(HALO):
            work[d] += edge_z[d]
            work[d, :8] += corner[d, :8]

    values = work[...].reshape(PLANES * plane_y, MESH)
    top, low = two_parts(values)
    right = jnp.concatenate([top, top, low], axis=1)
    start = pl.multiple_of(me[0] * (2 * MESH // nx), 2 * MESH // nx)
    result = dot_nt(table[pl.ds(start, 2 * MESH), :], right)
    for j in range(nx):
        for c in range(chunks):
            at = (j * chunks + c) * 2 * WAVES
            outs[c * nx + j][...] = result[at : at + 2 * WAVES]


def x_transform(me, mesh, edge_y, edge_z, corner, nx, plane_y, plane_z):
    chunks = MESH // nx // WAVES
    lanes = plane_y * plane_z
    width = PLANES * plane_y
    return pl.pallas_call(
        functools.partial(x_kernel, nx, chunks, plane_y),
        grid=(plane_z // PLANES,),
        in_specs=[
            pl.BlockSpec(memory_space=pltpu.SMEM),
            pl.BlockSpec((PLANES, plane_y, MESH), lambda i: (i, 0, 0)),
            pl.BlockSpec((HALO, PLANES, MESH), lambda i: (0, i, 0)),
            whole_block((HALO, plane_y, MESH)),
            whole_block((HALO, 16, MESH)),
            whole_block((4 * MESH, 3 * MESH)),
        ],
        out_specs=[pl.BlockSpec((2 * WAVES, width), lambda i: (0, i))] * (chunks * nx),
        out_shape=[jax.ShapeDtypeStruct((2 * WAVES, lanes), jnp.float32)] * (chunks * nx),
        scratch_shapes=[pltpu.VMEM((PLANES, plane_y, MESH), jnp.float32)],
        cost_estimate=pl.CostEstimate(
            flops=12 * MESH * MESH * lanes, bytes_accessed=6 * MESH * lanes, transcendentals=0
        ),
        name="along_x",
    )(
        me,
        mesh.reshape(plane_z, plane_y, MESH),
        edge_y.reshape(HALO, plane_z, MESH),
        edge_z.reshape(HALO, plane_y, MESH),
        corner.reshape(HALO, 16, MESH),
        jnp.asarray(x_table(nx)),
    )


def y_kernel(nx, ny, plane_y, me, *rest):
    blocks = rest[:nx]
    top_table, low_table = rest[nx], rest[nx + 1]
    outs = rest[nx + 2 : nx + 2 + ny]
    table, work = rest[nx + 2 + ny :]
    width = top_table.shape[3]

    @pl.when(pl.program_id(0) == 0)
    def _():
        start = pl.multiple_of(lax.rem(nx - me[0], nx) * plane_y, plane_y)
        for part, source in enumerate((top_table, low_table, top_table)):
            for j in range(ny):
                dest = lax.rem(me[1] + j, ny)
                for c in range(2):
                    at = part * 2 * MESH + c * MESH
                    table[at : at + MESH, j * width : (j + 1) * width] = source[
                        dest, c, pl.ds(start, MESH), :
                    ]

    per = 128 // plane_y
    lane = lax.broadcasted_iota(jnp.int32, (2 * WAVES, 128), 1) // plane_y

    def choose(pieces):
        result = pieces[0]
        for b in range(1, per):
            result = jnp.where(lane == b, pieces[b], result)
        return result

    for group in range(PLANES // per):
        for half in range(nx // per):
            held = [blocks[half * per + i][:, group * 128 : (group + 1) * 128] for i in range(per)]
            turned = []
            for r in range(per):
                mixed = choose([held[(b + r) % per] for b in range(per)])
                turned.append(pltpu.roll(mixed, r * plane_y, 1) if r else mixed)
            for l in range(per):
                row = choose([turned[(b - l) % per] for b in range(per)])
                at = (group * per + l) * WAVES
                for c in range(2):
                    column = c * MESH + half * 128
                    work[at : at + WAVES, column : column + 128] = row[
                        c * WAVES : (c + 1) * WAVES
                    ]
    top, low = two_parts(work[...])
    left = jnp.concatenate([top, top, low], axis=1)
    result = jnp.dot(left, table[...], preferred_element_type=jnp.float32)
    for j in range(ny):
        outs[j][...] = result[:, j * width : (j + 1) * width]


def y_transform(me, blocks, tables, nx, ny, plane_y, plane_z):
    width = 2 * MESH // ny
    rows = PLANES * WAVES
    return pl.pallas_call(
        functools.partial(y_kernel, nx, ny, plane_y),
        grid=(plane_z // PLANES,),
        in_specs=[pl.BlockSpec(memory_space=pltpu.SMEM)]
        + [pl.BlockSpec((2 * WAVES, PLANES * plane_y), lambda i: (0, i))] * nx
        + [whole_block(t.shape) for t in tables],
        out_specs=[pl.BlockSpec((rows, width), lambda i: (i, 0))] * ny,
        out_shape=[jax.ShapeDtypeStruct((plane_z * WAVES, width), jnp.float32)] * ny,
        scratch_shapes=[
            pltpu.VMEM((6 * MESH, 2 * MESH), jnp.bfloat16),
            pltpu.VMEM((rows, 2 * MESH), jnp.float32),
        ],
        cost_estimate=pl.CostEstimate(
            flops=24 * MESH * MESH * plane_z * WAVES,
            bytes_accessed=16 * MESH * plane_z * WAVES,
            transcendentals=0,
        ),
        name="along_y",
    )(me, *blocks, *tables)


def z_kernel(ny, plane_z, chunk, first, *rest):
    me, blocks = rest[0], rest[1 : 1 + ny]
    top_table, low_table, influence, shells = rest[1 + ny : 5 + ny]
    rest = rest[5 + ny :]
    if not first:
        old_sums, old_bins = rest[1:3]
        rest = rest[3:]
    out, sums, bins, table, work = rest
    k = pl.program_id(0)
    rows = MESH // ny

    @pl.when(k == 0)
    def _():
        start = pl.multiple_of(lax.rem(ny - me[1], ny) * plane_z, plane_z)
        for part, source in enumerate((top_table, low_table, top_table)):
            table[part * MESH : (part + 1) * MESH, :] = source[pl.ds(start, MESH), :]
        for wave in range(WAVES):
            for j in range(ny):
                work[wave, j * plane_z : (j + 1) * plane_z, :] = blocks[j][:, wave, :]
        if first:
            sums[...] = jnp.zeros_like(sums)
            bins[...] = jnp.zeros_like(bins)
        else:
            sums[...] = old_sums[...]
            bins[...] = old_bins[...]

    top, low = two_parts(work[k].T)
    left = jnp.concatenate([top, top, low], axis=1)
    mixed = jnp.dot(left, table[...], preferred_element_type=jnp.float32)
    real = mixed[:rows, :MESH] + mixed[rows:, MESH:]
    imag = mixed[rows:, :MESH] - mixed[:rows, MESH:]

    def wave(index):
        return jnp.where(index < MESH // 2, index, index - MESH).astype(jnp.float32)

    full = (rows, MESH)
    wave_x = wave(jnp.full(full, me[2] + chunk * WAVES + k, jnp.int32))
    wave_y = wave(lax.broadcasted_iota(jnp.int32, full, 0) + me[1] * rows)
    wave_z = wave(lax.broadcasted_iota(jnp.int32, full, 1))
    squared = wave_x * wave_x + wave_y * wave_y + wave_z * wave_z
    weight = jnp.where(squared > 0.0, influence[0], 0.0)
    out[0, 0] = weight * real
    out[1, 0] = weight * imag
    power = real * real + imag * imag
    weighted = weight * power
    coef = weighted * (2.0 + squared * (2.0 / SCREEN)) / jnp.maximum(squared, 1.0)

    def fold(values):
        return jnp.sum(values.reshape(rows // 8, 8, MESH), axis=0)

    plain = fold(coef)
    once = fold(coef * wave_y)
    twice = fold(coef * wave_y * wave_y)
    x8, z8 = wave_x[:8], wave_z[:8]
    sums[0] += fold(weighted)
    sums[1] += x8 * x8 * plain
    sums[2] += x8 * once
    sums[3] += x8 * z8 * plain
    sums[4] += twice
    sums[5] += z8 * once
    sums[6] += z8 * z8 * plain

    label = shells[0]
    high, low_label = label // SIDE, label % SIDE
    big = power.astype(jnp.bfloat16).astype(jnp.float32)
    small = power - big
    total = None
    for g in range(rows // 8):
        here = slice(g * 8, (g + 1) * 8)
        h, l, b, s = high[here], low_label[here], big[here], small[here]
        left = jnp.concatenate(
            [jnp.where(h == i, b, 0.0) for i in range(SIDE)]
            + [jnp.where(h == i, s, 0.0) for i in range(SIDE)],
            axis=0,
        ).astype(jnp.bfloat16)
        right = jnp.concatenate(
            [jnp.where(l == i, 1.0, 0.0) for i in range(SIDE)], axis=0
        ).astype(jnp.bfloat16)
        piece = dot_nt(left, right)
        total = piece if total is None else total + piece
    bins[...] += total


def z_transform(me, blocks, tables, influence, shells, carried, chunk, ny, plane_z, kx_rows):
    rows = MESH // ny
    first = carried is None
    shape = (2, kx_rows, rows, MESH)
    per_wave = pl.BlockSpec((1, rows, MESH), lambda k: (chunk * WAVES + k, 0, 0))
    specs = [pl.BlockSpec(memory_space=pltpu.SMEM)]
    specs += [whole_block((plane_z, WAVES, 2 * rows))] * ny
    specs += [whole_block(t.shape) for t in tables]
    specs += [per_wave, per_wave]
    values = [me, *(b.reshape(plane_z, WAVES, 2 * rows) for b in blocks), *tables]
    values += [influence, shells]
    aliases = {}
    if not first:
        aliases = {len(values): 0}
        specs += [pl.BlockSpec(memory_space=pl.ANY)]
        specs += [whole_block((8, 8, MESH)), whole_block((2 * SIDE * 8, SIDE * 8))]
        values += list(carried)
    return pl.pallas_call(
        functools.partial(z_kernel, ny, plane_z, chunk, first),
        grid=(WAVES,),
        in_specs=specs,
        out_specs=[
            pl.BlockSpec((2, 1, rows, MESH), lambda k: (0, chunk * WAVES + k, 0, 0)),
            whole_block((8, 8, MESH)),
            whole_block((2 * SIDE * 8, SIDE * 8)),
        ],
        out_shape=[
            jax.ShapeDtypeStruct(shape, jnp.float32),
            jax.ShapeDtypeStruct((8, 8, MESH), jnp.float32),
            jax.ShapeDtypeStruct((2 * SIDE * 8, SIDE * 8), jnp.float32),
        ],
        scratch_shapes=[
            pltpu.VMEM((3 * MESH, 2 * MESH), jnp.bfloat16),
            pltpu.VMEM((WAVES, MESH, 2 * rows), jnp.float32),
        ],
        input_output_aliases=aliases,
        cost_estimate=pl.CostEstimate(
            flops=24 * MESH * MESH * rows * WAVES,
            bytes_accessed=16 * MESH * rows * WAVES,
            transcendentals=0,
        ),
        name="along_z",
    )(*values)


def shifted(block, axes, size, distance):
    route = [(i, (i + distance) % size) for i in range(size)]
    return lax.ppermute(block, axes, route)


def shards(cells, fractions, charges, influence, shells):
    nx = lax.axis_size("gx")
    ny = lax.axis_size("gy")
    plane_y = MESH // nx
    plane_z = MESH // ny
    kx_rows = MESH // nx
    chunks = kx_rows // WAVES
    mine_x = lax.axis_index("gx").astype(jnp.int32)
    mine_y = lax.axis_index("gy").astype(jnp.int32)
    me = jnp.stack([mine_x, mine_y, mine_x * kx_rows])
    charges = charges.reshape(1, -1)
    xt, edge_y, edge_z, corner = edges(me, cells, fractions, charges, plane_y, plane_z)
    edge_y = shifted(edge_y, "gx", nx, 1)
    edge_z = shifted(edge_z, "gy", ny, 1)
    route = [
        (i * ny + j, (i + 1) % nx * ny + (j + 1) % ny) for i in range(nx) for j in range(ny)
    ]
    corner = lax.ppermute(corner, ("gx", "gy"), route)
    mesh = spread(me, cells, fractions, xt, plane_y, plane_z)
    along_x = x_transform(me, mesh, edge_y, edge_z, corner, nx, plane_y, plane_z)
    tables_y = [jnp.asarray(t) for t in y_table(nx, ny)]
    tables_z = [jnp.asarray(t) for t in z_table(ny)]
    arrived = []
    for c in range(chunks):
        blocks = along_x[c * nx : (c + 1) * nx]
        blocks = [b if j == 0 else shifted(b, "gx", nx, j) for j, b in enumerate(blocks)]
        blocks = y_transform(me, blocks, tables_y, nx, ny, plane_y, plane_z)
        arrived.append([b if j == 0 else shifted(b, "gy", ny, j) for j, b in enumerate(blocks)])
    carried = None
    for c in range(chunks):
        carried = z_transform(
            me, arrived[c], tables_z, influence, shells, carried, c, ny, plane_z, kx_rows
        )
    potential_hat, sums, bins = carried
    row = lax.broadcasted_iota(jnp.int32, bins.shape, 0) % 8
    column = lax.broadcasted_iota(jnp.int32, bins.shape, 1) % 8
    bins = jnp.where(row == column, bins, 0.0).reshape(2, SIDE, 8, SIDE * 8).sum((0, 2))
    sums = sums.reshape(8, 8, 2, 128).sum((1, 2))
    both = jnp.concatenate([bins, sums], axis=0)
    for axis, size in (("gx", nx), ("gy", ny)):
        step = 1
        while step < size:
            route = [(i, i ^ step) for i in range(size)]
            both = both + lax.ppermute(both, axis, route)
            step *= 2
    spectrum = both[:SIDE].reshape(SIDE, SIDE, 8).sum(2).reshape(SHELLS) * (SHELLS / MESH**3)
    sums = both[SIDE:].sum(1)
    scale = 0.5 / MESH**3
    energy = scale * sums[0]
    cross = jnp.stack([sums[i] for i in (1, 2, 3, 2, 4, 5, 3, 5, 6)]).reshape(3, 3)
    virial = scale * (jnp.eye(3, dtype=jnp.float32) * sums[0] - cross)
    return (potential_hat, energy, virial, spectrum)


def solution(mesh):
    return jax.shard_map(
        shards,
        mesh=mesh,
        in_specs=(
            P(None, ("gx", "gy")),
            P(None, ("gx", "gy")),
            P(("gx", "gy")),
            P("gx", "gy", None),
            P("gx", "gy", None),
        ),
        out_specs=(P(None, "gx", "gy", None), P(), P(), P()),
        check_vma=False,
    )
```

```python
import functools

import jax
import jax.numpy as jnp
import numpy as np
from jax import lax
from jax.experimental import pallas as pl
from jax.experimental.pallas import tpu as pltpu
from jax.sharding import PartitionSpec as P

MESH = 256
SHELLS = 256
SCREEN = 4096
HALO = 3
WAVES = 8
PLANES = 16
SIDE = 16
BLOCK = 2048
GROUP = 32
TOGETHER = 4


def whole_block(shape):
    return pl.BlockSpec(shape, lambda *_: (0,) * len(shape))


def two_parts(values):
    top = values.astype(jnp.bfloat16)
    return top, (values - top.astype(jnp.float32)).astype(jnp.bfloat16)


def table_parts(table):
    top = np.asarray(table, np.float32).astype(jnp.bfloat16)
    rest = (table - top.astype(np.float64)).astype(np.float32).astype(jnp.bfloat16)
    return top, rest


def waves():
    index = np.arange(MESH)
    angle = (index[:, None] * index[None, :] % MESH) * (2.0 * np.pi / MESH)
    return np.cos(angle) / np.sqrt(MESH), np.sin(angle) / np.sqrt(MESH)


def x_table(nx, first, chunks):
    cosine, sine = waves()
    both = np.stack([cosine, -sine]).reshape(2, nx, MESH // nx // WAVES, WAVES, MESH)
    both = both[:, :, first : first + chunks]
    rows = both.transpose(1, 2, 0, 3, 4).reshape(-1, MESH)
    top, rest = table_parts(rows)
    return np.concatenate([top, rest, top], axis=1)


def y_table(ny):
    cosine, sine = waves()
    width = MESH // ny
    full = np.stack([np.stack([cosine, -sine], 1), np.stack([sine, cosine], 1)])
    full = full.reshape(2, MESH, 2, ny, width).transpose(3, 0, 1, 2, 4)
    full = full.reshape(ny, 2, MESH, 2 * width)
    return table_parts(full.reshape(ny, 2 * MESH, 2 * width))


def z_table():
    return table_parts(np.concatenate(waves(), axis=1))


def spline(frac):
    cube = frac * frac * frac
    square = frac * frac
    rest = 1.0 - frac
    return (
        rest * rest * rest / 6.0,
        (3.0 * cube - 6.0 * square + 4.0) / 6.0,
        (-3.0 * cube + 3.0 * square + 3.0 * frac + 1.0) / 6.0,
        cube / 6.0,
    )


def placed(offset, weights):
    result = jnp.where(offset == 3, weights[3], 0.0)
    for turn in (2, 1, 0):
        result = jnp.where(offset == turn, weights[turn], result)
    return result


def axis_table(cell, weights, axis, rows, first):
    count = cell.shape[1]
    index = lax.broadcasted_iota(jnp.int32, (rows, count), 0)
    offset = index - (cell[axis : axis + 1, :] - first)
    return placed(offset, [w[axis : axis + 1, :] for w in weights])


NT = (((1,), (1,)), ((), ()))


def dot_nt(a, b):
    return lax.dot_general(a, b, NT, preferred_element_type=jnp.float32)


def x_factor(cell, weights):
    count = cell.shape[1]
    rows = lax.broadcasted_iota(jnp.int32, (16, count), 0).astype(jnp.float32)
    offset = (rows - cell.astype(jnp.float32)).astype(jnp.bfloat16)
    values = [jnp.broadcast_to(w, (16, count)).astype(jnp.bfloat16) for w in weights]
    zero = jnp.zeros((16, count), jnp.bfloat16)
    tiles = []
    for first in range(0, MESH, 16):
        tile = zero
        for turn in range(4):
            tile = jnp.where(offset == jnp.bfloat16(turn - first), values[turn], tile)
            if first == 0 and turn:
                tile = jnp.where(offset == jnp.bfloat16(turn - MESH), values[turn], tile)
        tiles.append(tile)
    return tiles


def pair_rows(pairs, at, one, many):
    size = many.shape[0]
    pairs[at : at + size, :] = (one * many).astype(jnp.bfloat16)
    return at + size


def add_groups(out, pairs, table_y, zt, plane_y, planes, xt, group):
    for first in range(0, planes, group):
        at = first * plane_y
        for z in range(first, first + group):
            at = pair_rows(pairs, at, zt[z : z + 1, :], table_y)
        rows = slice(first * plane_y, (first + group) * plane_y)
        out[rows, :] += dot_nt(pairs[rows, :], xt[...])


def upper_kernel(plane_y, plane_z, me, coming, ahead, charge, cells, frac, xt, *rest):
    out, edge_y, edge_z, corner, zt, pairs, rows, held = rest

    @pl.when(pl.program_id(0) == 0)
    def _():
        held[...] = jnp.zeros_like(held)
        out[...] = jnp.zeros_like(out)
        edge_y[...] = jnp.zeros_like(edge_y)
        edge_z[...] = jnp.zeros_like(edge_z)
        corner[...] = jnp.zeros_like(corner)

    charged = charge[...]
    weights = [charged * w for w in spline(ahead[0:1, :])]
    tiles = x_factor(coming[0:1, :], weights)
    for k, tile in enumerate(tiles):
        xt[k * 16 : (k + 1) * 16, :] = tile

    cell = cells[...]
    weights = spline(frac[...])
    yt = axis_table(cell, weights, 1, plane_y + 16, me[0] * plane_y)
    zt[...] = axis_table(cell, weights, 2, plane_z + 8, me[1] * plane_z)
    table_y = yt[:plane_y]
    half = plane_z // 2
    add_groups(out, pairs, table_y, zt.at[half:], plane_y, half, held, min(GROUP, half))
    at = 0
    for d in range(HALO):
        at = pair_rows(rows, at, yt[plane_y + d : plane_y + d + 1, :], zt[:plane_z, :])
    for d in range(HALO):
        at = pair_rows(rows, at, zt[plane_z + d : plane_z + d + 1, :], table_y)
    for d in range(HALO):
        at = pair_rows(rows, at, zt[plane_z + d : plane_z + d + 1, :], yt[plane_y:])
    total = dot_nt(rows[...], held[...])
    at = HALO * plane_z
    edge_y[...] += total[:at]
    edge_z[...] += total[at : at + HALO * plane_y]
    corner[...] += total[at + HALO * plane_y :]
    held[...] = xt[...]


def lower_kernel(plane_y, plane_z, me, cells, frac, xt, held, out, zt, pairs):
    del held
    cell = cells[...]
    weights = spline(frac[...])
    table_y = axis_table(cell, weights, 1, plane_y, me[0] * plane_y)
    zt[...] = axis_table(cell, weights, 2, plane_z // 2, me[1] * plane_z)

    @pl.when(pl.program_id(0) == 0)
    def _():
        out[...] = jnp.zeros_like(out)

    add_groups(out, pairs, table_y, zt, plane_y, plane_z // 2, xt, min(GROUP, plane_z // 2))


def atom_specs(block):
    return [
        pl.BlockSpec(memory_space=pltpu.SMEM),
        pl.BlockSpec((3, block), lambda i: (0, i)),
        pl.BlockSpec((3, block), lambda i: (0, i)),
    ]


def spread_upper(me, cells, frac, charges, plane_y, plane_z):
    atoms = charges.shape[1]
    block = min(BLOCK, atoms)
    turns = atoms // block
    half = plane_y * plane_z // 2
    rows = HALO * (plane_z + plane_y + 16)
    sizes = (HALO * plane_z, HALO * plane_y, HALO * 16)

    def ahead(i):
        return (0, jnp.minimum(i, turns - 1))

    def behind(i):
        return (0, jnp.maximum(i - 1, 0))

    return pl.pallas_call(
        functools.partial(upper_kernel, plane_y, plane_z),
        grid=(turns + 1,),
        in_specs=[
            pl.BlockSpec(memory_space=pltpu.SMEM),
            pl.BlockSpec((3, block), ahead),
            pl.BlockSpec((3, block), ahead),
            pl.BlockSpec((1, block), ahead),
            pl.BlockSpec((3, block), behind),
            pl.BlockSpec((3, block), behind),
        ],
        out_specs=[
            pl.BlockSpec((MESH, block), ahead),
            pl.BlockSpec((half, MESH), lambda i: (1, 0)),
        ]
        + [whole_block((n, MESH)) for n in sizes],
        out_shape=[
            jax.ShapeDtypeStruct((MESH, atoms), jnp.bfloat16),
            jax.ShapeDtypeStruct((2 * half, MESH), jnp.float32),
        ]
        + [jax.ShapeDtypeStruct((n, MESH), jnp.float32) for n in sizes],
        scratch_shapes=[
            pltpu.VMEM((plane_z + 8, block), jnp.float32),
            pltpu.VMEM((half, block), jnp.bfloat16),
            pltpu.VMEM((rows, block), jnp.bfloat16),
            pltpu.VMEM((MESH, block), jnp.bfloat16),
        ],
        cost_estimate=pl.CostEstimate(
            flops=3 * half * atoms * MESH, bytes_accessed=4 * MESH * atoms, transcendentals=0
        ),
        name="spread_upper",
    )(me, cells, frac, charges, cells, frac)


def spread_lower(me, cells, frac, xt, mesh, plane_y, plane_z):
    atoms = cells.shape[1]
    block = min(BLOCK, atoms)
    half = plane_y * plane_z // 2
    return pl.pallas_call(
        functools.partial(lower_kernel, plane_y, plane_z),
        grid=(atoms // block,),
        in_specs=atom_specs(block)
        + [pl.BlockSpec((MESH, block), lambda i: (0, i)), pl.BlockSpec(memory_space=pl.ANY)],
        out_specs=pl.BlockSpec((half, MESH), lambda i: (0, 0)),
        out_shape=jax.ShapeDtypeStruct((2 * half, MESH), jnp.float32),
        scratch_shapes=[
            pltpu.VMEM((plane_z // 2, block), jnp.float32),
            pltpu.VMEM((half, block), jnp.bfloat16),
        ],
        input_output_aliases={4: 0},
        cost_estimate=pl.CostEstimate(
            flops=2 * half * atoms * MESH, bytes_accessed=4 * MESH * atoms, transcendentals=0
        ),
        name="spread_lower",
    )(me, cells, frac, xt, mesh)


def x_kernel(nx, chunks, plane_y, mesh, edge_y, edge_z, corner, table, *rest):
    outs, work = rest[:-1], rest[-1]
    work[...] = mesh[...]
    for d in range(HALO):
        work[:, d, :] += edge_y[d]

    @pl.when(pl.program_id(0) == 0)
    def _():
        for d in range(HALO):
            work[d] += edge_z[d]
            work[d, :8] += corner[d, :8]

    values = work[...].reshape(PLANES * plane_y, MESH)
    top, low = two_parts(values)
    right = jnp.concatenate([top, top, low], axis=1)
    result = dot_nt(table[...], right)
    for j in range(nx):
        for c in range(chunks):
            at = (j * chunks + c) * 2 * WAVES
            outs[c][j] = result[at : at + 2 * WAVES]


def x_transform(mesh, edge_y, edge_z, corner, nx, plane_y, plane_z, first, chunks):
    table = jnp.asarray(x_table(nx, first, chunks))
    lanes = plane_y * plane_z
    width = PLANES * plane_y
    return pl.pallas_call(
        functools.partial(x_kernel, nx, chunks, plane_y),
        grid=(plane_z // PLANES,),
        in_specs=[
            pl.BlockSpec((PLANES, plane_y, MESH), lambda i: (i, 0, 0)),
            pl.BlockSpec((HALO, PLANES, MESH), lambda i: (0, i, 0)),
            whole_block((HALO, plane_y, MESH)),
            whole_block((HALO, 16, MESH)),
            whole_block(table.shape),
        ],
        out_specs=[pl.BlockSpec((nx, 2 * WAVES, width), lambda i: (0, 0, i))] * chunks,
        out_shape=[jax.ShapeDtypeStruct((nx, 2 * WAVES, lanes), jnp.float32)] * chunks,
        scratch_shapes=[pltpu.VMEM((PLANES, plane_y, MESH), jnp.float32)],
        cost_estimate=pl.CostEstimate(
            flops=2 * table.size * lanes, bytes_accessed=6 * MESH * lanes, transcendentals=0
        ),
        name="along_x",
    )(
        mesh.reshape(plane_z, plane_y, MESH),
        edge_y.reshape(HALO, plane_z, MESH),
        edge_z.reshape(HALO, plane_y, MESH),
        corner.reshape(HALO, 16, MESH),
        table,
    )


def y_kernel(nx, ny, plane_y, blocks, table, *rest):
    outs, work = rest[:-1], rest[-1]
    width = 2 * MESH // ny
    per = 128 // plane_y
    lane = lax.broadcasted_iota(jnp.int32, (2 * WAVES, 128), 1) // plane_y

    def choose(pieces):
        result = pieces[0]
        for b in range(1, per):
            result = jnp.where(lane == b, pieces[b], result)
        return result

    for group in range(PLANES // per):
        for half in range(nx // per):
            held = [blocks[half * per + i, :, group * 128 : (group + 1) * 128] for i in range(per)]
            turned = []
            for r in range(per):
                mixed = choose([held[(b + r) % per] for b in range(per)])
                turned.append(pltpu.roll(mixed, r * plane_y, 1) if r else mixed)
            for l in range(per):
                row = choose([turned[(b - l) % per] for b in range(per)])
                at = (group * per + l) * WAVES
                for c in range(2):
                    column = c * MESH + half * 128
                    work[at : at + WAVES, column : column + 128] = row[
                        c * WAVES : (c + 1) * WAVES
                    ]
    top, low = two_parts(work[...])
    left = jnp.concatenate([top, top, low], axis=1)
    result = jnp.dot(left, table[...], preferred_element_type=jnp.float32)
    for j in range(ny):
        outs[j][...] = result[:, j * width : (j + 1) * width]


def y_transform(blocks, table, nx, ny, plane_y, plane_z):
    width = 2 * MESH // ny
    rows = PLANES * WAVES
    return pl.pallas_call(
        functools.partial(y_kernel, nx, ny, plane_y),
        grid=(plane_z // PLANES,),
        in_specs=[
            pl.BlockSpec((nx, 2 * WAVES, PLANES * plane_y), lambda i: (0, 0, i)),
            whole_block(table.shape),
        ],
        out_specs=[pl.BlockSpec((rows, width), lambda i: (i, 0))] * ny,
        out_shape=[jax.ShapeDtypeStruct((plane_z * WAVES, width), jnp.float32)] * ny,
        scratch_shapes=[pltpu.VMEM((rows, 2 * MESH), jnp.float32)],
        cost_estimate=pl.CostEstimate(
            flops=24 * MESH * MESH * plane_z * WAVES,
            bytes_accessed=16 * MESH * plane_z * WAVES,
            transcendentals=0,
        ),
        name="along_y",
    )(blocks, table)


def turn_kernel(ny, plane_z, me, top_y, low_y, top_z, low_z, table_y, table_z):
    width = 2 * MESH // ny
    for part, source in enumerate((top_y, low_y, top_y)):
        for j in range(ny):
            dest = lax.rem(me[1] + j, ny)
            table_y[part * 2 * MESH : (part + 1) * 2 * MESH, j * width : (j + 1) * width] = source[
                dest
            ]
    for part, source in enumerate((top_z, low_z, top_z)):
        for j in range(ny):
            start = pl.multiple_of(lax.rem(me[1] + ny - j, ny) * plane_z, plane_z)
            at = part * MESH + j * plane_z
            table_z[at : at + plane_z, :] = source[pl.ds(start, plane_z), :]


def turned_tables(me, ny, plane_z):
    tables = [jnp.asarray(t) for t in (*y_table(ny), *z_table())]
    return pl.pallas_call(
        functools.partial(turn_kernel, ny, plane_z),
        in_specs=[pl.BlockSpec(memory_space=pltpu.SMEM)]
        + [pl.BlockSpec(memory_space=pltpu.VMEM)] * 4,
        out_specs=[pl.BlockSpec(memory_space=pltpu.VMEM)] * 2,
        out_shape=[
            jax.ShapeDtypeStruct((6 * MESH, 2 * MESH), jnp.bfloat16),
            jax.ShapeDtypeStruct((3 * MESH, 2 * MESH), jnp.bfloat16),
        ],
        name="turned_tables",
    )(me, *tables)


def z_kernel(ny, plane_z, chunk, first, last, *rest):
    me, blocks = rest[0], rest[1 : 1 + ny]
    table, influence, shells = rest[1 + ny : 4 + ny]
    rest = rest[4 + ny :]
    if not first:
        old_sums, old_bins = rest[1:3]
        rest = rest[3:]
    out, sums, bins, done, work = rest
    k = pl.program_id(0)
    rows = MESH // ny

    @pl.when(k == 0)
    def _():
        for wave in range(WAVES):
            for j in range(ny):
                work[wave, j * plane_z : (j + 1) * plane_z, :] = blocks[j][
                    pl.ds(wave, plane_z, stride=WAVES), :
                ]
        if first:
            sums[...] = jnp.zeros_like(sums)
            bins[...] = jnp.zeros_like(bins)
        else:
            sums[...] = old_sums[...]
            bins[...] = old_bins[...]

    def wave(index):
        return jnp.where(index < MESH // 2, index, index - MESH).astype(jnp.float32)

    def fold(values):
        return jnp.sum(values.reshape(rows // 8, 8, MESH), axis=0)

    full = (rows, MESH)
    zero, unit = jnp.bfloat16(0), jnp.bfloat16(1)
    total = None
    for t in range(TOGETHER):
        top, low = two_parts(work[k * TOGETHER + t].T)
        left = jnp.concatenate([top, top, low], axis=1)
        mixed = jnp.dot(left, table[...], preferred_element_type=jnp.float32)
        real = mixed[:rows, :MESH] + mixed[rows:, MESH:]
        imag = mixed[rows:, :MESH] - mixed[:rows, MESH:]

        wave_x = wave(jnp.full(full, me[2] + chunk * WAVES + k * TOGETHER + t, jnp.int32))
        wave_y = wave(lax.broadcasted_iota(jnp.int32, full, 0) + me[1] * rows)
        wave_z = wave(lax.broadcasted_iota(jnp.int32, full, 1))
        squared = wave_x * wave_x + wave_y * wave_y + wave_z * wave_z
        weight = jnp.where(squared > 0.0, influence[t], 0.0)
        out[0, t] = weight * real
        out[1, t] = weight * imag
        power = real * real + imag * imag
        weighted = weight * power
        coef = weighted * (2.0 + squared * (2.0 / SCREEN)) / jnp.maximum(squared, 1.0)

        plain = fold(coef)
        once = fold(coef * wave_y)
        twice = fold(coef * wave_y * wave_y)
        x8, z8 = wave_x[:8], wave_z[:8]
        sums[0] += fold(weighted)
        sums[1] += x8 * x8 * plain
        sums[2] += x8 * once
        sums[3] += x8 * z8 * plain
        sums[4] += twice
        sums[5] += z8 * once
        sums[6] += z8 * z8 * plain

        label = shells[t]
        high = (label >> 4).astype(jnp.float32).astype(jnp.bfloat16)
        low_label = (label & 15).astype(jnp.float32).astype(jnp.bfloat16)
        big, small = two_parts(power)
        for g in range(rows // 16):
            here = slice(g * 16, (g + 1) * 16)
            h, l, b, s = high[here], low_label[here], big[here], small[here]
            names = [jnp.bfloat16(i) for i in range(SIDE)]
            left = jnp.concatenate(
                [jnp.where(h == i, b, zero) for i in names] + [jnp.where(h == i, s, zero) for i in names],
                axis=0,
            )
            right = jnp.concatenate([jnp.where(l == i, unit, zero) for i in names], axis=0)
            piece = dot_nt(left, right)
            total = piece if total is None else total + piece
    bins[...] += total

    @pl.when(k == (WAVES // TOGETHER - 1 if last else WAVES))
    def _():
        row = lax.broadcasted_iota(jnp.int32, bins.shape, 0)
        column = lax.broadcasted_iota(jnp.int32, bins.shape, 1)
        kept = jnp.where((row & 15) == (column & 15), bins[...], 0.0)
        kept = jnp.sum(kept.reshape(2, SIDE, SIDE, SIDE * SIDE), axis=(0, 2))
        done[:SIDE] = kept[:, :128]
        done[SIDE : 2 * SIDE] = kept[:, 128:]
        parts = jnp.sum(sums[...], axis=1)
        done[2 * SIDE :] = parts[:, :128] + parts[:, 128:]


def z_transform(me, blocks, table, influence, shells, carried, chunk, ny, plane_z, kx_rows):
    rows = MESH // ny
    first = carried is None
    last = (chunk + 1) * WAVES == kx_rows
    bins = (2 * SIDE * SIDE, SIDE * SIDE)
    shape = (2, kx_rows, rows, MESH)
    turns = WAVES // TOGETHER
    per_wave = pl.BlockSpec((TOGETHER, rows, MESH), lambda k: (chunk * turns + k, 0, 0))
    specs = [pl.BlockSpec(memory_space=pltpu.SMEM)]
    specs += [whole_block((plane_z * WAVES, 2 * rows))] * ny
    specs += [whole_block(table.shape), per_wave, per_wave]
    values = [me, *blocks, table]
    values += [influence, shells]
    aliases = {}
    if not first:
        aliases = {len(values): 0}
        specs += [pl.BlockSpec(memory_space=pl.ANY)]
        specs += [whole_block((8, 8, MESH)), whole_block(bins)]
        values += list(carried[:3])
    return pl.pallas_call(
        functools.partial(z_kernel, ny, plane_z, chunk, first, last),
        grid=(WAVES // TOGETHER,),
        in_specs=specs,
        out_specs=[
            pl.BlockSpec((2, TOGETHER, rows, MESH), lambda k: (0, chunk * turns + k, 0, 0)),
            whole_block((8, 8, MESH)),
            whole_block(bins),
            whole_block((2 * SIDE + 8, 128)),
        ],
        out_shape=[
            jax.ShapeDtypeStruct(shape, jnp.float32),
            jax.ShapeDtypeStruct((8, 8, MESH), jnp.float32),
            jax.ShapeDtypeStruct(bins, jnp.float32),
            jax.ShapeDtypeStruct((2 * SIDE + 8, 128), jnp.float32),
        ],
        scratch_shapes=[pltpu.VMEM((WAVES, MESH, 2 * rows), jnp.float32)],
        input_output_aliases=aliases,
        cost_estimate=pl.CostEstimate(
            flops=24 * MESH * MESH * rows * WAVES,
            bytes_accessed=16 * MESH * rows * WAVES,
            transcendentals=0,
        ),
        name="along_z",
    )(*values)


def shifted(block, axes, size, distance):
    route = [(i, (i + distance) % size) for i in range(size)]
    return lax.ppermute(block, axes, route)


def reciprocal(cells, fractions, charges, influence, shells):
    nx = lax.axis_size("gx")
    ny = lax.axis_size("gy")
    plane_y = MESH // nx
    plane_z = MESH // ny
    kx_rows = MESH // nx
    chunks = kx_rows // WAVES
    mine_x = lax.axis_index("gx").astype(jnp.int32)
    mine_y = lax.axis_index("gy").astype(jnp.int32)
    me = jnp.stack([mine_x, mine_y, mine_x * kx_rows])
    charges = charges.reshape(1, -1)
    xt, mesh, edge_y, edge_z, corner = spread_upper(
        me, cells, fractions, charges, plane_y, plane_z
    )
    edge_y = shifted(edge_y, "gx", nx, 1)
    edge_z = shifted(edge_z, "gy", ny, 1)
    route = [
        (i * ny + j, (i + 1) % nx * ny + (j + 1) % ny) for i in range(nx) for j in range(ny)
    ]
    corner = lax.ppermute(corner, ("gx", "gy"), route)
    mesh = spread_lower(me, cells, fractions, xt, mesh, plane_y, plane_z)
    mesh = (mesh, edge_y, edge_z, corner)
    along_x = x_transform(*mesh, nx, plane_y, plane_z, 0, 1)
    along_x += x_transform(*mesh, nx, plane_y, plane_z, 1, chunks - 1)
    table_y, table_z = turned_tables(me, ny, plane_z)
    arrived = []
    for c in range(chunks):
        blocks = lax.all_to_all(along_x[c], "gx", 0, 0, tiled=True)
        blocks = y_transform(blocks, table_y, nx, ny, plane_y, plane_z)
        arrived.append(
            [b if j == 0 else shifted(b, "gy", ny, j) for j, b in enumerate(blocks)]
        )
    carried = None
    for c in range(chunks):
        carried = z_transform(
            me, arrived[c], table_z, influence, shells, carried, c, ny, plane_z, kx_rows
        )
    potential_hat, both = carried[0], carried[3]
    for axis, size in (("gx", nx), ("gy", ny)):
        step = 1
        while step < size:
            route = [(i, i ^ step) for i in range(size)]
            both = both + lax.ppermute(both, axis, route)
            step *= 2
    bins = both[: 2 * SIDE].reshape(2, SIDE, 8, SIDE).sum(3).transpose(1, 0, 2)
    spectrum = bins.reshape(SHELLS) * (SHELLS / MESH**3)
    sums = both[2 * SIDE :].sum(1)
    scale = 0.5 / MESH**3
    energy = scale * sums[0]
    cross = jnp.stack([sums[i] for i in (1, 2, 3, 2, 4, 5, 3, 5, 6)]).reshape(3, 3)
    virial = scale * (jnp.eye(3, dtype=jnp.float32) * sums[0] - cross)
    return (potential_hat, energy, virial, spectrum)


def solution(mesh):
    return jax.shard_map(
        reciprocal,
        mesh=mesh,
        in_specs=(
            P(None, ("gx", "gy")),
            P(None, ("gx", "gy")),
            P(("gx", "gy")),
            P("gx", "gy", None),
            P("gx", "gy", None),
        ),
        out_specs=(P(None, "gx", "gy", None), P(), P(), P()),
        check_vma=False,
    )
```
